32 devices in a mesh: expert: 8 (over z, y), tensor: 4 (over x, core).
Axes of the slice: x: 2, y: 2, z: 4, core: 2. Of those that a mesh axis runs over, the one named last changes fastest.
Arguments:
- tokens: bfloat16 [1024, 3072], P('expert', 'tensor'), may hold values from -6 to 6
- expert_ids: int32 [1024, 2], P('expert'), may hold values from 0 to 7, all different within a row; in each aligned block of 128 rows (0 to 127, 128 to 255, ...) at most 48 rows name the same one
- joined_weight: bfloat16 [8, 3072, 2, 16384], P('expert', 'tensor'), may hold values from -0.109375 to 0.109375
Outputs:
- hidden: bfloat16 [1024, 2, 1, 16384], P('expert', None, None, 'tensor')
The draws below stay inside these ranges and needn't reach their ends.
Inputs may be any that keep to these rules, and one draw needn't show every extreme that they name: `expert_ids`: each row names 2 different experts. Among the rows of one device (each aligned block of 128 rows) no expert is named by more than 48 rows, and in some blocks one expert is named by exactly 48 rows.
All inputs are finite; a program needn't handle non-finite values.
Results may differ from the reference program's by a relative error of at most 0.001.
Values may be sent and summed in bfloat16 or wider, within the bound.
A program may use at most 256 MiB of HBM per device.

```python
import math
import jax
import jax.numpy as jnp
import numpy as np
from jax import lax

E = 8
TOP = 2
D = 3072
FF = 16384
TOK_DEV = 128
CAP = 48
REP = 1
FB = 16384
EB = 8
TOKENS = 1024


def levels(own_key, dims, cuts, low, high):
    loudness = 1.0
    for dim, blocks in cuts:
        steps = jax.random.uniform(jax.random.fold_in(jax.random.fold_in(own_key, 6), dim), (blocks,), jnp.float32, low / len(cuts), high / len(cuts))
        loudness = loudness * jnp.repeat(jnp.exp(steps), dims[dim] // blocks).reshape((-1,) + (1,) * (len(dims) - 1 - dim))
    return loudness


def shared_out(key, own, number, rows, amount, top, bound, lean):
    order = jax.random.permutation(key, amount)
    crowded, usual = load_shares(amount, rows * top, bound, lean, True), load_shares(amount, rows * top, bound, lean, False)
    places = jnp.arange(amount)

    def named(tallies, rotation):
        used = int((tallies > 0).sum())
        fixed = max(1, used // 4)
        passed = fixed + (places - fixed + rotation * (used - fixed)) % max(1, amount - fixed)
        return jnp.zeros((amount,), jnp.int32).at[order[jnp.where(places < fixed, places, passed)]].set(jnp.asarray(tallies, jnp.int32))

    tallies = jnp.where(number % 4 == 0, named(crowded, number // 4), named(usual, number - number // 4 - 1))
    mixed = jax.random.permutation(jax.random.fold_in(own, 3), amount)
    giver, sink = mixed[0:amount // 2 * 2:2], mixed[1:amount // 2 * 2:2]
    margin = jnp.minimum(tallies[giver] - 1, bound - tallies[sink]) // 2
    margin = jnp.where((giver == order[0]) | (sink == order[0]) | (tallies[sink] == 0), 0, jnp.maximum(margin, 0))
    passed = jax.random.randint(jax.random.fold_in(own, 4), (amount // 2,), 0, 1 << 20) % (margin + 1)
    tallies = tallies.at[giver].add(-passed).at[sink].add(passed)
    labels = jnp.searchsorted(jnp.cumsum(tallies), jnp.arange(rows * top), side="right").astype(jnp.int32)
    listing = labels.reshape(top, rows).T
    listing = listing[jax.random.permutation(jax.random.fold_in(own, 1), rows)]
    rotation = jax.random.randint(jax.random.fold_in(own, 2), (rows, 1), 0, top)
    return jnp.take_along_axis(listing, (jnp.arange(top)[None, :] + rotation) % top, axis=1)


def load_shares(amount, total, bound, lean, full):
    portions = [(1 << 20) // math.isqrt(standing ** lean) + 1 for standing in range(1, amount + 1)]
    largest = bound if full else min(bound, max(-(-total // amount), total * portions[0] // sum(portions)))
    least = 1 if total - largest >= amount - 1 else 0
    holding, spare = [largest] + [least] * (amount - 1), total - largest - least * (amount - 1)
    while spare > 0:
        free = [i for i in range(1, amount) if holding[i] < largest] or [i for i in range(1, amount) if holding[i] < bound]
        mass, remaining = sum([portions[i] for i in free]), spare
        for i in free:
            addition = min(bound - holding[i], max(1, remaining * portions[i] // mass), spare)
            holding[i] = holding[i] + addition
            spare = spare - addition
    return np.array(holding)


def gaussian(rng, shape, deviation, reach, split=(), kind=jnp.bfloat16):
    drawn = jax.random.normal(rng, shape, jnp.float32) * deviation
    if len(split) > 0:
        drawn = levels(rng, shape, split, -0.22, 0.18) * drawn
    return jnp.clip(drawn, min=-reach, max=reach).astype(kind)


def setup_inputs(seed: int = 0) -> dict:
    key_of = jax.random.split(jax.random.key(seed), 4)
    tokens = gaussian(key_of[0], (TOKENS, D), 1.0, 6.0, ((0, 8), (1, 4)))
    expert_ids_keys = jax.random.split(jax.random.fold_in(key_of[1], 1), TOKENS // TOK_DEV)
    expert_ids_turns = jax.random.permutation(jax.random.fold_in(key_of[1], 3), TOKENS // TOK_DEV)
    expert_ids = jax.vmap(lambda own, number: shared_out(jax.random.fold_in(key_of[1], 2), own, number, TOK_DEV, E, TOP, CAP, 2))(expert_ids_keys, expert_ids_turns).reshape((TOKENS, TOP))
    joined_weight = gaussian(key_of[2], (EB, D, 2, FB), D ** -0.5, 0.109375, ((0, 8), (1, 4)))
    return {"tokens": tokens, "expert_ids": expert_ids, "joined_weight": joined_weight}


def reference(tokens, expert_ids, joined_weight):
    sources = TOKENS // TOK_DEV
    flat_ids = expert_ids.reshape(sources, TOK_DEV * TOP)
    chosen = (flat_ids[:, :, None] == jnp.arange(E, dtype=jnp.int32)[None, None, :]).astype(jnp.int32)
    earlier = jnp.cumsum(chosen, axis=1) - chosen
    position = jnp.sum(earlier * chosen, axis=2).astype(jnp.int32)
    slot_index = (jnp.arange(sources, dtype=jnp.int32)[:, None] * CAP + position).reshape(-1).astype(jnp.int32)
    all_ids = flat_ids.reshape(-1)
    token_of = (jnp.arange(TOKENS * TOP, dtype=jnp.int32) // TOP).astype(jnp.int32)
    routed = tokens[token_of]

    def one_expert(index, result):
        expert = jnp.asarray(index).astype(jnp.int32)
        w_block = lax.dynamic_slice_in_dim(joined_weight, (expert * REP).astype(jnp.int32), REP, 0)
        weight = jnp.transpose(w_block, (1, 2, 0, 3)).reshape(D, 2 * FF)
        is_mine = all_ids == expert
        target = jnp.where(is_mine, slot_index, sources * CAP).astype(jnp.int32)
        buffer = jnp.zeros((sources * CAP + 1, D), jnp.bfloat16).at[target].set(routed)
        gate_up = jnp.dot(buffer, weight, preferred_element_type=jnp.float32)
        active = (jax.nn.silu(gate_up[:, :FF]) * gate_up[:, FF:]).astype(jnp.bfloat16)
        return jnp.where(is_mine[:, None], active[target], result)

    start_out = jnp.zeros((TOKENS * TOP, FF), jnp.bfloat16)
    result = lax.fori_loop(0, E, one_expert, start_out)
    return result.reshape(TOKENS, TOP, REP, FB)
```

```python
import jax
import jax.numpy as jnp
from jax import lax
from jax.sharding import PartitionSpec as P

E = 8
TOP = 2
CAP = 48
CHUNKS = 4
TOP_CODE = 32767.0


def local(tokens, expert_ids, joined_weight):
    groups = lax.axis_size("tensor")
    blocks = lax.axis_size("expert")
    copies = blocks // E
    me = lax.axis_index("tensor")
    core, chip = me % 2, me // 2
    chips = groups // 2
    rows = joined_weight.shape[1]
    half = joined_weight.shape[3] // groups
    chunk = half // CHUNKS if half % (CHUNKS * 128) == 0 else half
    count = half // chunk
    weight = joined_weight[0]
    swap = [(i, i ^ 1) for i in range(groups)]

    def columns(owner, j):
        piece = lax.dynamic_slice(weight, (0, 0, owner * half + j * chunk), (rows, 2, chunk))
        return jnp.concatenate([piece[:, 0], piece[:, 1]], axis=1)

    order = [(o, j) for o in list(range(1, chips)) + [0] for j in range(count)]
    given = {}
    for o, j in order:
        target = (chip + o) % chips
        given[o, j] = lax.ppermute(columns(target * 2 + 1 - core, j), "tensor", swap)

    tok_count, width = tokens.shape
    flat_ids = expert_ids.reshape(-1)
    chosen = (flat_ids[:, None] == jnp.arange(E, dtype=jnp.int32)[None, :]).astype(jnp.int32)
    earlier = jnp.cumsum(chosen, axis=0) - chosen
    position = jnp.sum(earlier * chosen, axis=1)
    slot_index = flat_ids * CAP + position
    pick_table = (slot_index[:, None] == jnp.arange(E * CAP, dtype=jnp.int32)[None, :]).astype(
        jnp.bfloat16
    )
    token_table = pick_table.reshape(tok_count, TOP, E * CAP).sum(axis=1)
    placed = lax.dot_general(
        token_table, tokens, (((0,), (0,)), ((), ())), preferred_element_type=jnp.float32
    )
    placed = placed.astype(jnp.bfloat16).reshape(E, 1, CAP, width)
    outgoing = jnp.broadcast_to(placed, (E, copies, CAP, width)).reshape(blocks, CAP, width)
    received = lax.all_to_all(outgoing, "expert", split_axis=0, concat_axis=0, tiled=True)
    own = received.reshape(blocks * CAP, width)
    other = lax.ppermute(own, "tensor", swap)

    def partial(o, j):
        target = (chip + o) % chips
        kept = columns(target * 2 + core, j)
        return jnp.dot(own, kept, preferred_element_type=jnp.float32) + jnp.dot(
            other, given[o, j], preferred_element_type=jnp.float32
        )

    arrived = {}
    for o, j in order:
        if o == 0:
            continue
        part = partial(o, j)
        top = jnp.maximum(jnp.max(jnp.abs(part), axis=1), 1e-30)
        code = jnp.round(part * (TOP_CODE / top)[:, None]).astype(jnp.int16)
        ahead = [(i, (i + 2 * o) % groups) for i in range(groups)]
        arrived[o, j] = (
            lax.ppermute(code, "tensor", ahead),
            lax.ppermute(top * (1.0 / TOP_CODE), "tensor", ahead),
        )

    outs = []
    for j in range(count):
        gate_up = partial(0, j)
        for o in range(1, chips):
            code, step = arrived[o, j]
            gate_up = gate_up + code.astype(jnp.float32) * step[:, None]
        active = (jax.nn.silu(gate_up[:, :chunk]) * gate_up[:, chunk:]).astype(jnp.bfloat16)
        returned = lax.all_to_all(
            active.reshape(blocks, CAP, chunk), "expert", split_axis=0, concat_axis=0, tiled=True
        )
        grouped = (
            returned.reshape(E, copies, CAP, chunk)
            .transpose(0, 2, 1, 3)
            .reshape(E * CAP, copies * chunk)
        )
        hidden = jnp.dot(pick_table, grouped, preferred_element_type=jnp.float32)
        outs.append(hidden.astype(jnp.bfloat16).reshape(tok_count, TOP, copies, chunk))
    return jnp.concatenate(outs, axis=3)


def solution(mesh):
    placed = (P("expert", "tensor"), P("expert", None), P("expert", "tensor", None, None))
    return jax.shard_map(
        local,
        mesh=mesh,
        in_specs=placed,
        out_specs=P("expert", None, None, "tensor"),
        check_vma=False,
    )
```

```python
import jax
import jax.numpy as jnp
from jax import lax
from jax.sharding import PartitionSpec as P

E = 8
TOP = 2
CAP = 48
CHUNKS = 4
TOP_CODE = 32767.0


def local(tokens, expert_ids, joined_weight):
    groups = lax.axis_size("tensor")
    blocks = lax.axis_size("expert")
    copies = blocks // E
    me = lax.axis_index("tensor")
    core, chip = me % 2, me // 2
    chips = groups // 2
    rows = joined_weight.shape[1]
    half = joined_weight.shape[3] // groups
    chunk = half // CHUNKS if half % (CHUNKS * 128) == 0 else half
    count = half // chunk
    swap = [(i, i ^ 1) for i in range(groups)]

    def columns(weight, owner, j):
        piece = lax.dynamic_slice(
            weight, (0, 0, 0, owner * half + j * chunk), (1, rows, 2, chunk)
        )[0]
        return piece.transpose(1, 0, 2)

    tok_count, width = tokens.shape
    flat_ids = expert_ids.reshape(-1)
    chosen = (flat_ids[:, None] == jnp.arange(E, dtype=jnp.int32)[None, :]).astype(jnp.int32)
    earlier = jnp.cumsum(chosen, axis=0) - chosen
    position = jnp.sum(earlier * chosen, axis=1)
    slot_index = flat_ids * CAP + position
    pick_table = (slot_index[:, None] == jnp.arange(E * CAP, dtype=jnp.int32)[None, :]).astype(
        jnp.bfloat16
    )
    token_table = pick_table.reshape(tok_count, TOP, E * CAP).sum(axis=1)
    placed = lax.dot_general(
        token_table, tokens, (((0,), (0,)), ((), ())), preferred_element_type=jnp.float32
    )
    placed = placed.astype(jnp.bfloat16).reshape(E, 1, CAP, width)
    outgoing = jnp.broadcast_to(placed, (E, copies, CAP, width)).reshape(blocks, CAP, width)
    received = lax.all_to_all(outgoing, "expert", split_axis=0, concat_axis=0, tiled=True)
    own = received.reshape(blocks * CAP, width)
    other = lax.ppermute(own, "tensor", swap)

    order = [(o, j) for o in list(range(1, chips)) + [0] for j in range(count)]
    weight = joined_weight
    given, kept = {}, {}

    def take(index, source):
        o, j = order[index]
        target = (chip + o) % chips
        given[o, j] = lax.ppermute(columns(source, target * 2 + 1 - core, j), "tensor", swap)
        kept[o, j] = columns(source, target * 2 + core, j)

    take(0, weight)
    arrived, base = {}, {}
    for index, (o, j) in enumerate(order):
        if index + 1 < len(order):
            take(index + 1, weight)
        mine, theirs = kept[o, j], given[o, j]
        parts = [
            jnp.dot(own, mine[c], preferred_element_type=jnp.float32)
            + jnp.dot(other, theirs[c], preferred_element_type=jnp.float32)
            for c in range(2)
        ]
        if o == 0:
            base[j] = parts
            continue
        ahead = [(i, (i + 2 * o) % groups) for i in range(groups)]
        codes, steps = [], []
        for part in parts:
            top = jnp.maximum(jnp.max(jnp.abs(part), axis=1), 1e-30)
            codes.append(jnp.round(part * (TOP_CODE / top)[:, None]).astype(jnp.int16))
            steps.append(top * (1.0 / TOP_CODE))
        codes[0], codes[1], steps[0], steps[1], weight, own, other = lax.optimization_barrier(
            (codes[0], codes[1], steps[0], steps[1], weight, own, other)
        )
        step = lax.ppermute(jnp.stack(steps), "tensor", ahead)
        arrived[o, j] = [
            (lax.ppermute(codes[c], "tensor", ahead), step[c]) for c in range(2)
        ]

    outs = []
    for j in range(count):
        gate, up = base[j]
        for o in range(1, chips):
            (gate_code, gate_step), (up_code, up_step) = arrived[o, j]
            gate = gate + gate_code.astype(jnp.float32) * gate_step[:, None]
            up = up + up_code.astype(jnp.float32) * up_step[:, None]
        active = (jax.nn.silu(gate) * up).astype(jnp.bfloat16)
        returned = lax.all_to_all(
            active.reshape(blocks, CAP, chunk), "expert", split_axis=0, concat_axis=0, tiled=True
        )
        grouped = (
            returned.reshape(E, copies, CAP, chunk)
            .transpose(0, 2, 1, 3)
            .reshape(E * CAP, copies * chunk)
        )
        hidden = jnp.dot(pick_table, grouped, preferred_element_type=jnp.float32)
        outs.append(hidden.astype(jnp.bfloat16).reshape(tok_count, TOP, copies, chunk))
    return jnp.concatenate(outs, axis=3)


def solution(mesh):
    placed = (P("expert", "tensor"), P("expert", None), P("expert", "tensor", None, None))
    return jax.shard_map(
        local,
        mesh=mesh,
        in_specs=placed,
        out_specs=P("expert", None, None, "tensor"),
        check_vma=False,
    )
```
